256 devices in a mesh: seq: 64 (over x, z_hi, y, core), head: 4 (over z_lo).
Axes of the slice: x: 4, y: 4, z: 8 (z_hi: 2, z_lo: 4; z = z_hi * 4 + z_lo), core: 2. Of those that a mesh axis runs over, the one named last changes fastest.
Arguments:
- span_order: int32 [128], replicated, may hold values from 0 to 127, each once
- queries: bfloat16 [8192, 36864], P('seq', 'head'), may hold values from -32 to 32
- latent_kv: bfloat16 [8192, 576], P(('seq', 'head')), may hold values from -8 to 8
- w_uv: bfloat16 [64, 512, 128], P('head'), may hold values from -0.25 to 0.25
Outputs:
- attended: bfloat16 [8192, 8192], P('seq', 'head')
The draws below stay inside these ranges and needn't reach their ends.
Inputs may be any that keep to these rules, and one draw needn't show every extreme that they name: `span_order`: each of 0 to 127 appears once.
All inputs are finite; a program needn't handle non-finite values.
Results may differ from the reference program's by a relative error of at most 0.0065.
Values may be sent and summed in bfloat16 or wider, within the bound.
No kernel may reach another device: no remote copies, remote signals or barrier semaphores. Data moves between devices by JAX's collectives and lax.ppermute only.
A program may use at most 128 MiB of HBM per device.

```python
import math
import jax
import jax.numpy as jnp
from jax import lax

HEADS = 64
KV_RANK = 512
ROPE_DIM = 64
NOPE_DIM = 128
V_DIM = 128
QK_DIM = 576
TOK_DEV = 128
SEQS = 2
TOKENS = 8192
SEQ_LEN = 4096
SPANS = 128


def draw_latent_kv(key, part):
    drawn = jnp.clip(jax.random.normal(jax.random.fold_in(key, 1), (TOKENS, QK_DIM), jnp.float32), -6.0, 6.0)
    return drawn.astype(jnp.bfloat16)


def draw_queries(key, part):
    drawn = jnp.clip(jax.random.normal(jax.random.fold_in(key, 21), (TOKENS, HEADS, QK_DIM), jnp.float32), -6.0, 6.0)
    return drawn.reshape(TOKENS, HEADS * QK_DIM).astype(jnp.bfloat16)


def levels(rng, extent, split, low, high):
    def one(position, blocks):
        draws = jax.random.uniform(jax.random.fold_in(jax.random.fold_in(rng, 6), position), (blocks,), jnp.float32, low / len(split), high / len(split))
        return jnp.repeat(jnp.exp(draws), extent[position] // blocks).reshape((-1,) + (1,) * (len(extent) - position - 1))

    factor_of = one(*split[0])
    for cut in split[1:]:
        factor_of = factor_of * one(*cut)
    return factor_of


def noise(own_key, shape, spread, reach, pieces=(), kind=jnp.bfloat16):
    values = spread * jax.random.normal(own_key, shape, jnp.float32)
    if pieces:
        values = values * levels(own_key, shape, pieces, -0.22, 0.18)
    return jnp.clip(values, -reach, reach).astype(kind)


def setup_inputs(seed: int = 0) -> dict:
    arg_keys = jax.random.split(jax.random.key(seed), 5)
    return {
        "span_order": jax.random.permutation(arg_keys[0], SPANS).astype(jnp.int32),
        "queries": draw_queries(jax.random.fold_in(arg_keys[4], 71), 0),
        "latent_kv": draw_latent_kv(jax.random.fold_in(arg_keys[4], 71), 0),
        "w_uv": noise(arg_keys[3], (HEADS, KV_RANK, V_DIM), KV_RANK ** -0.5, 0.25, ((0, 4),)),
    }


theta_base = 10000.0


def angle_tables(positions, half_width):
    inverse_freq = jnp.exp(-math.log(theta_base) * jnp.arange(half_width, dtype=jnp.float32) / half_width)
    phases = positions.astype(jnp.float32)[:, None] * inverse_freq[None, :]
    return jnp.cos(phases), jnp.sin(phases)


def rotate(values, cosine, sine_table):
    half_width = values.shape[-1] // 2
    lower_part = values[..., :half_width]
    upper_part = values[..., half_width:]
    return jnp.concatenate([lower_part * cosine - upper_part * sine_table, upper_part * cosine + lower_part * sine_table], -1)


def reference(span_order, queries, latent_kv, w_uv):
    span_len = TOK_DEV // 2
    stream_ids = (span_order[:, None] * span_len + jnp.arange(span_len, dtype=jnp.int32)[None, :]).reshape(-1).astype(jnp.int32)
    positions = stream_ids % SEQ_LEN
    cosine, sine_table = angle_tables(positions, ROPE_DIM // 2)
    key_rows = jnp.concatenate([latent_kv[:, :KV_RANK], rotate(latent_kv[:, KV_RANK:].astype(jnp.float32), cosine, sine_table).astype(jnp.bfloat16)], 1)
    sorted_rows = jnp.argsort(stream_ids).astype(jnp.int32)
    ordered_key_rows = lax.optimization_barrier(key_rows[sorted_rows]).astype(jnp.float32).reshape(SEQS, SEQ_LEN, QK_DIM)
    ordered_value_rows = ordered_key_rows[..., :KV_RANK]
    query_grid = queries.reshape(TOKENS, HEADS, QK_DIM)
    causal = jnp.arange(SEQ_LEN)[:, None] >= jnp.arange(SEQ_LEN)[None, :]
    logit_scale_factor = (NOPE_DIM + ROPE_DIM) ** -0.5

    def one_head(head_index):
        query_head = lax.dynamic_index_in_dim(query_grid, head_index, 1, keepdims=False)
        rotated = rotate(query_head[:, KV_RANK:].astype(jnp.float32), cosine, sine_table).astype(jnp.bfloat16)
        query_head = jnp.concatenate([query_head[:, :KV_RANK], rotated], 1)
        ordered_query_rows = lax.optimization_barrier(query_head[sorted_rows]).astype(jnp.float32).reshape(SEQS, SEQ_LEN, QK_DIM)
        logit_scores = jnp.einsum("xpa,xfa->xpf", ordered_query_rows, ordered_key_rows) * logit_scale_factor
        logit_scores = jnp.where(causal[None], logit_scores, -jnp.inf)
        row_top = jnp.max(logit_scores, -1, keepdims=True)
        expo = jnp.exp(logit_scores - row_top)
        totals = jnp.sum(expo, -1)
        softmax_weights = lax.optimization_barrier(expo.astype(jnp.bfloat16)).astype(jnp.float32)
        numerator_sums = jnp.einsum("mzw,mwi->mzi", softmax_weights, ordered_value_rows)
        latent_out = lax.optimization_barrier((numerator_sums / totals[..., None]).astype(jnp.bfloat16)).astype(jnp.float32)
        weight_head = lax.dynamic_index_in_dim(w_uv, head_index, 0, keepdims=False).astype(jnp.float32)
        projected = jnp.einsum("bqr,rv->bqv", latent_out, weight_head).astype(jnp.bfloat16)
        return projected.reshape(TOKENS, V_DIM)[stream_ids]

    outputs = lax.map(one_head, jnp.arange(HEADS, dtype=jnp.int32))
    return jnp.moveaxis(outputs, 0, 1).reshape(TOKENS, HEADS * V_DIM)
```

```python
import functools
import math

import jax
import jax.numpy as jnp
from jax import lax
from jax.experimental import pallas as pl
from jax.experimental.pallas import tpu as pltpu
from jax.sharding import PartitionSpec as P

ROPE_DIM = 64
NOPE_DIM = 128
SEQS = 2
AXES = ("seq", "head")
NX, NY, NZ, NC = 4, 4, 8, 2
ZL = 4
SPAN = 64
SLOTS = 4
TILE = SLOTS * SPAN
THETA = 10000.0

SHIFTS = {"own": 0, "up": -1, "down": 1, "far": 2}


def place(x, y, z, c):
    return (((x * (NZ // ZL) + z // ZL) * NY + y) * NC + c) * ZL + z % ZL


def chips():
    return [(x, y, z, c) for x in range(NX) for y in range(NY) for z in range(NZ) for c in range(NC)]


def permute(value, target):
    pairs = [(place(*d), place(*target(*d))) for d in chips()]
    return lax.ppermute(value, AXES, pairs)


def second_axis(step):
    return lambda x, y, z, c: ((x + step) % NX, y, z, c) if c == 1 else (x, (y + step) % NY, z, c)


def other_core(x, y, z, c):
    return (x, y, z, 1 - c)


GROUP_Z = [[place(x, y, z, c) for z in range(NZ)] for x in range(NX) for y in range(NY) for c in range(NC)]
GROUP_A = [[place(x, y, z, 0) for x in range(NX)] for y in range(NY) for z in range(NZ)] + [
    [place(x, y, z, 1) for y in range(NY)] for x in range(NX) for z in range(NZ)
]


def collect(shard, groups):
    n = len(groups[0])
    copies = jnp.broadcast_to(shard[None], (n, *shard.shape))
    tiles = lax.all_to_all(copies, AXES, split_axis=0, concat_axis=0, tiled=True, axis_index_groups=groups)
    return tiles.reshape(n * shard.shape[0], *shard.shape[1:])


def angle_tables(positions, half_width):
    inverse_freq = jnp.exp(-math.log(THETA) * jnp.arange(half_width, dtype=jnp.float32) / half_width)
    phases = positions.astype(jnp.float32)[:, None] * inverse_freq[None, :]
    return (jnp.cos(phases), jnp.sin(phases))


def rotate(values, cosine, sine_table):
    half = values.shape[-1] // 2
    lo, hi = values[..., :half], values[..., half:]
    return jnp.concatenate([lo * cosine - hi * sine_table, hi * cosine + lo * sine_table], -1)


CHUNKS = (
    (("mine", "own"), ("peer", "own")),
    (("mine", "up"), ("mine", "down"), ("peer", "up"), ("peer", "down")),
    (("mine", "far"), ("peer", "far")),
)
SPANS_PER_PIECE = 16
PIECE_ROWS = SPANS_PER_PIECE * SPAN
VMEM_LIMIT = 20 << 20
LIST_PAD = 8
SHARD = 32
PACK = SHARD * 576 // 128


def list_len(chunk):
    return len(chunk) * SPANS_PER_PIECE + LIST_PAD


def plan_kernel(order_ref, here_ref, *lists):
    x, y, core, seq = here_ref[0], here_ref[1], here_ref[2], here_ref[3]
    mine = [order_ref[2 * seq + q] for q in range(2)]
    floors = [jnp.bitwise_and(g, -64) for g in mine]
    for chunk, out in zip(CHUNKS, lists):
        length = list_len(chunk)
        counts = [jnp.int32(0), jnp.int32(0)]
        diags = [jnp.int32(0), jnp.int32(0)]
        for n, (side, name) in enumerate(chunk):
            on = core if side == "mine" else 1 - core
            fixed_x = jnp.bitwise_and(x + (SHIFTS[name] + NX), NX - 1)
            fixed_y = jnp.bitwise_and(y + (SHIFTS[name] + NY), NY - 1)
            base = jnp.where(on == 0, fixed_y * 4, fixed_x * 32 + 2)
            stride = jnp.where(on == 0, 32, 4)
            for a in range(4):
                start = base + stride * a
                for zp in range(4):
                    g = order_ref[start + (zp // 2) * 16 + zp % 2]
                    row = n * SPANS_PER_PIECE + a * 4 + zp
                    for q in range(2):
                        out[q * length + counts[q]] = row
                        full = jnp.logical_and(g >= floors[q], g < mine[q])
                        counts[q] = counts[q] + full.astype(jnp.int32)
                        diags[q] = jnp.where(g == mine[q], row, diags[q])
        for q in range(2):
            for k in range(LIST_PAD):
                out[q * length + counts[q] + k] = diags[q] if k == 0 else 0
            out[2 * length + q] = counts[q]


def plan(order, here):
    smem = pl.BlockSpec(memory_space=pltpu.SMEM)
    return pl.pallas_call(
        plan_kernel,
        out_shape=[jax.ShapeDtypeStruct((2 * list_len(ch) + 2,), jnp.int32) for ch in CHUNKS],
        in_specs=[smem, smem],
        out_specs=[smem] * len(CHUNKS),
        name="plan",
    )(order, here)


def turn(pair, cosine, sine_table):
    lane = lax.broadcasted_iota(jnp.int32, pair.shape, pair.ndim - 1)
    swapped = jnp.where(
        jnp.bitwise_and(lane, 32) == 0,
        pltpu.roll(pair, 96, pair.ndim - 1),
        pltpu.roll(pair, 32, pair.ndim - 1),
    )
    return pair * cosine + swapped * sine_table


def prepare_kernel(queries_ref, cos_ref, sin_ref, out_ref):
    rows = queries_ref.shape[0]
    span_rows = rows // 2
    width = out_ref.shape[2]
    rank = width - ROPE_DIM
    cosine, sine_table = cos_ref[...], sin_ref[...]
    lane = lax.broadcasted_iota(jnp.int32, (rows, 128), 1)
    low = lane < 64
    for pair in range(queries_ref.shape[1] // (2 * width)):
        at = 2 * width * pair

        def block(k, at=at):
            return queries_ref[:, at + 128 * k : at + 128 * (k + 1)]

        blocks = [block(k) for k in range(2 * width // 128)]
        mid = rank // 128
        shifted = [pltpu.roll(b.astype(jnp.float32), 64, 1) for b in blocks[mid:]]
        ropes = jnp.where(low, blocks[mid].astype(jnp.float32), blocks[-1].astype(jnp.float32))
        ropes = turn(ropes, cosine, sine_table)
        tails = [ropes.astype(jnp.bfloat16), pltpu.roll(ropes, 64, 1).astype(jnp.bfloat16)]
        bodies = [
            blocks[:mid],
            [jnp.where(low, shifted[k], shifted[k + 1]).astype(jnp.bfloat16) for k in range(mid)],
        ]
        for odd in range(2):
            head = 2 * pair + odd
            for q in range(2):
                part = slice(q * span_rows, (q + 1) * span_rows)
                dst = slice(head * span_rows, (head + 1) * span_rows)
                for k in range(mid):
                    out_ref[q, dst, 128 * k : 128 * (k + 1)] = bodies[odd][k][part]
                out_ref[q, dst, rank:width] = tails[odd][part, :ROPE_DIM]


def prepare(queries, cosine, sine_table, heads):
    vmem = pl.BlockSpec(memory_space=pltpu.VMEM)
    rows, lanes = queries.shape
    width = lanes // heads
    return pl.pallas_call(
        prepare_kernel,
        out_shape=jax.ShapeDtypeStruct((2, heads * rows // 2, width), jnp.bfloat16),
        in_specs=[vmem] * 3,
        out_specs=vmem,
        cost_estimate=pl.CostEstimate(flops=4 << 30, bytes_accessed=6 << 20, transcendentals=0),
        compiler_params=pltpu.CompilerParams(vmem_limit_bytes=16 << 20),
        name="prepare",
    )(queries, cosine, sine_table)


def attend_kernel(n_pieces, first, last, scale, *refs):
    refs = list(refs)
    lists, q_ref = refs.pop(0), refs.pop(0)
    pieces = [refs.pop(0) for _ in range(n_pieces)]
    if not first:
        acc_in, top_in, tot_in = refs.pop(0), refs.pop(0), refs.pop(0)
    if last:
        w_ref, out_ref = refs.pop(0), refs.pop(0)
        acc_ref, top_ref, tot_ref = acc_in, top_in, tot_in
    else:
        acc_ref, top_ref, tot_ref = refs.pop(0), refs.pop(0), refs.pop(0)
    kbuf, rope_buf, s_buf, sems = refs
    shards = PIECE_ROWS // SHARD
    rank = kbuf.shape[2] - ROPE_DIM
    rows = q_ref.shape[1]
    copies = []
    for i, piece in enumerate(pieces):
        own = []
        dst = pl.ds(i * shards, shards)
        for b in range(rank // 128):
            own.append(
                pltpu.make_async_copy(
                    piece.at[:, pl.ds(b * SHARD, SHARD), :], kbuf.at[dst, :, pl.ds(b * 128, 128)], sems.at[i, b]
                )
            )
        own.append(
            pltpu.make_async_copy(
                piece.at[:, pl.ds(rank // 128 * SHARD, SHARD // 2), :], rope_buf.at[dst], sems.at[i, rank // 128]
            )
        )
        copies.append(own)
    for own in copies:
        for cp in own:
            cp.start()
    if first:
        acc_ref[...] = jnp.zeros_like(acc_ref)
        top_ref[...] = jnp.full_like(top_ref, -jnp.inf)
        tot_ref[...] = jnp.zeros_like(tot_ref)
    for i, own in enumerate(copies):
        for cp in own:
            cp.wait()
        dst = pl.ds(i * shards, shards)
        packed = rope_buf[dst]
        kbuf[dst, pl.ds(0, SHARD // 2), pl.ds(rank, ROPE_DIM)] = packed[:, :, :ROPE_DIM]
        kbuf[dst, pl.ds(SHARD // 2, SHARD // 2), pl.ds(rank, ROPE_DIM)] = packed[:, :, ROPE_DIM:]

    length = n_pieces * SPANS_PER_PIECE + LIST_PAD
    counts = [lists[2 * length + q] for q in range(2)]
    extra = 1 if first else 0
    items = [lax.shift_right_logical(n + (extra + SLOTS - 1), 2) for n in counts]

    def locate(i):
        q = (i >= items[0]).astype(jnp.int32)
        return q, i - q * items[0]

    def keys(q, i):
        tiles = [kbuf[pl.ds(lists[q * length + i * SLOTS + k] * 2, 2)] for k in range(SLOTS)]
        return jnp.concatenate(tiles, 0).reshape(TILE, kbuf.shape[2])

    def score(i, slot):
        q, at = locate(i)
        s_buf[slot] = lax.dot_general(
            q_ref[q], keys(q, at), (((1,), (1,)), ((), ())), preferred_element_type=jnp.float32
        )

    cols = lax.broadcasted_iota(jnp.int32, (SPAN, TILE), 1)
    toks = lax.broadcasted_iota(jnp.int32, (SPAN, TILE), 0)
    ahead = cols - toks if first else cols + 1
    total_items = items[0] + items[1]

    @pl.when(total_items > 0)
    def _():
        score(0, 0)

    def step(i, carry):
        slot = jnp.bitwise_and(i, 1)
        score(i + 1, 1 - slot)
        q, at = locate(i)
        count = jnp.where(q == 0, counts[0], counts[1])
        visible = ahead <= SPAN * (count - SLOTS * at)
        values = keys(q, at)[:, :rank]
        probs, alphas = [], []
        for h in range(rows // SPAN):
            part = pl.ds(h * SPAN, SPAN)
            s = jnp.where(visible, s_buf[slot, part, :] * scale, -jnp.inf)
            old = top_ref[q, part, :]
            new = jnp.maximum(old, jnp.max(s, 1, keepdims=True))
            top_ref[q, part, :] = new
            alpha = jnp.exp2(old - new)
            p = jnp.exp2(s - jnp.concatenate([new] * (TILE // 128), 1))
            sums = p[:, :128]
            for b in range(1, TILE // 128):
                sums = sums + p[:, b * 128 : (b + 1) * 128]
            tot_ref[q, part, :] = tot_ref[q, part, :] * alpha + sums
            probs.append(p.astype(jnp.bfloat16))
            alphas.append(alpha)
        contrib = jnp.dot(jnp.concatenate(probs, 0), values, preferred_element_type=jnp.float32)
        alpha = jnp.concatenate(alphas, 0)
        for b in range(rank // 128):
            lanes = pl.ds(b * 128, 128)
            acc_ref[q, :, lanes] = acc_ref[q, :, lanes] * alpha + contrib[:, b * 128 : (b + 1) * 128]
        return carry

    lax.fori_loop(0, total_items, step, 0)
    if last:
        for q in range(2):
            for h in range(rows // SPAN):
                part = pl.ds(h * SPAN, SPAN)
                total = jnp.sum(tot_ref[q, part, :], 1, keepdims=True)
                latent = (acc_ref[q, part, :] / total).astype(jnp.bfloat16)
                out = jnp.dot(latent, w_ref[h], preferred_element_type=jnp.float32)
                out_ref[pl.ds(q * SPAN, SPAN), pl.ds(h * 128, 128)] = out.astype(jnp.bfloat16)


def attend(lists, q, pieces, state, w_uv, scale):
    first, last = state is None, w_uv is not None
    vmem = pl.BlockSpec(memory_space=pltpu.VMEM)
    smem = pl.BlockSpec(memory_space=pltpu.SMEM)
    hbm = pl.BlockSpec(memory_space=pl.ANY)
    spans, rows, width = q.shape
    rank = width - ROPE_DIM
    args = [lists, q, *pieces]
    in_specs = [smem, vmem] + [hbm] * len(pieces)
    aliases = {}
    if not first:
        if not last:
            aliases = {len(args) + k: k for k in range(3)}
        args += list(state)
        in_specs += [vmem] * 3
    if last:
        args.append(w_uv)
        in_specs.append(vmem)
        out_shape = jax.ShapeDtypeStruct((spans * SPAN, w_uv.shape[0] * w_uv.shape[2]), jnp.bfloat16)
        out_specs = vmem
    else:
        out_shape = [
            jax.ShapeDtypeStruct((spans, rows, rank), jnp.float32),
            jax.ShapeDtypeStruct((spans, rows, 128), jnp.float32),
            jax.ShapeDtypeStruct((spans, rows, 128), jnp.float32),
        ]
        out_specs = [vmem] * 3
    n = len(pieces)
    flops = n * rows * PIECE_ROWS * (width + rank) * 2
    return pl.pallas_call(
        functools.partial(attend_kernel, n, first, last, scale),
        out_shape=out_shape,
        in_specs=in_specs,
        out_specs=out_specs,
        scratch_shapes=[
            pltpu.VMEM((n * PIECE_ROWS // SHARD, SHARD, width), jnp.bfloat16),
            pltpu.VMEM((n * PIECE_ROWS // SHARD, SHARD // 2, 128), jnp.bfloat16),
            pltpu.VMEM((2, rows, TILE), jnp.float32),
            pltpu.SemaphoreType.DMA((n, rank // 128 + 1)),
        ],
        input_output_aliases=aliases,
        cost_estimate=pl.CostEstimate(flops=flops, bytes_accessed=8 << 20, transcendentals=n * rows * PIECE_ROWS),
        compiler_params=pltpu.CompilerParams(vmem_limit_bytes=VMEM_LIMIT),
        name="attend_" + ("first" if first else "last" if last else "middle"),
    )(*args)


def per_device(span_order, queries, latent_kv, w_uv):
    tok_dev = queries.shape[0]
    head_count, latent_rank, _ = w_uv.shape
    row_width = queries.shape[1] // head_count
    rope_width = row_width - latent_rank
    seq, head = lax.axis_index("seq"), lax.axis_index("head")
    core, y, x = seq % NC, (seq // NC) % NY, seq // (NC * NY * (NZ // ZL))
    seq_len = tok_dev * lax.axis_size("seq") // SEQS

    kv_count = latent_kv.shape[0]
    mine = lax.dynamic_slice_in_dim(span_order, 2 * seq, 2)
    positions = (mine[:, None] * SPAN + jnp.arange(SPAN, dtype=jnp.int32)[None, :]).reshape(-1) % seq_len
    cos_q, sin_q = angle_tables(positions, rope_width // 2)
    cos_k = lax.dynamic_slice_in_dim(cos_q, head * kv_count, kv_count)
    sin_k = lax.dynamic_slice_in_dim(sin_q, head * kv_count, kv_count)
    rope = rotate(latent_kv[:, latent_rank:].astype(jnp.float32), cos_k, sin_k).astype(jnp.bfloat16)
    packed = jnp.concatenate(
        [latent_kv[:, 128 * b : 128 * (b + 1)] for b in range(latent_rank // 128)]
        + [jnp.concatenate([rope[: kv_count // 2], rope[kv_count // 2 :]], 1)],
        0,
    )[None]
    got = {("mine", "own"): collect(collect(packed, GROUP_Z), GROUP_A)}
    own = got["mine", "own"]
    for name in ("up", "down", "far"):
        got["mine", name] = permute(own, second_axis(-SHIFTS[name]))
    got["peer", "own"] = permute(own, other_core)

    here = jnp.stack([x, y, core, seq]).astype(jnp.int32)
    lists = plan(span_order, here)
    q = prepare(
        queries,
        jnp.concatenate([cos_q] * 4, 1),
        jnp.concatenate([-sin_q, sin_q] * 2, 1),
        head_count,
    )

    scale = (NOPE_DIM + ROPE_DIM) ** -0.5 * math.log2(math.e)
    state = attend(lists[0], q, [got[key] for key in CHUNKS[0]], None, None, scale)
    for name in ("up", "down"):
        got["mine", name], state = lax.optimization_barrier((got["mine", name], state))
        got["peer", name] = permute(got["mine", name], other_core)
    state = attend(lists[1], q, [got[key] for key in CHUNKS[1]], state, None, scale)
    got["peer", "far"] = permute(got["mine", "far"], other_core)
    state = attend(lists[2], q, [got[key] for key in CHUNKS[2]], state, w_uv, scale)
    return state


def solution(mesh):
    in_specs = (P(), P("seq", "head"), P(("seq", "head"), None), P("head", None, None))
    return jax.shard_map(
        per_device, mesh=mesh, in_specs=in_specs, out_specs=P("seq", "head"), check_vma=False
    )
```

```python
import functools
import math

import jax
import jax.numpy as jnp
from jax import lax
from jax.experimental import pallas as pl
from jax.experimental.pallas import tpu as pltpu
from jax.sharding import PartitionSpec as P

ROPE_DIM = 64
NOPE_DIM = 128
SEQS = 2
AXES = ("seq", "head")
NX, NY, NZ, NC = 4, 4, 8, 2
ZL = 4
SPAN = 64
SLOTS = 4
TILE = SLOTS * SPAN
THETA = 10000.0

SHIFTS = {"own": 0, "up": -1, "down": 1, "far": 2}


def place(x, y, z, c):
    return (((x * (NZ // ZL) + z // ZL) * NY + y) * NC + c) * ZL + z % ZL


def chips():
    return [(x, y, z, c) for x in range(NX) for y in range(NY) for z in range(NZ) for c in range(NC)]


def permute(value, target):
    pairs = [(place(*d), place(*target(*d))) for d in chips()]
    return lax.ppermute(value, AXES, pairs)


def second_axis(step):
    return lambda x, y, z, c: ((x + step) % NX, y, z, c) if c == 1 else (x, (y + step) % NY, z, c)


def other_core(x, y, z, c):
    return (x, y, z, 1 - c)


GROUP_Z = [[place(x, y, z, c) for z in range(NZ)] for x in range(NX) for y in range(NY) for c in range(NC)]
GROUP_A = [[place(x, y, z, 0) for x in range(NX)] for y in range(NY) for z in range(NZ)] + [
    [place(x, y, z, 1) for y in range(NY)] for x in range(NX) for z in range(NZ)
]


def collect(shard, groups):
    n = len(groups[0])
    copies = jnp.broadcast_to(shard[None], (n, *shard.shape))
    tiles = lax.all_to_all(copies, AXES, split_axis=0, concat_axis=0, tiled=True, axis_index_groups=groups)
    return tiles.reshape(n * shard.shape[0], *shard.shape[1:])


def angle_tables(positions, half_width):
    inverse_freq = jnp.exp(-math.log(THETA) * jnp.arange(half_width, dtype=jnp.float32) / half_width)
    phases = positions.astype(jnp.float32)[:, None] * inverse_freq[None, :]
    return (jnp.cos(phases), jnp.sin(phases))


def rotate(values, cosine, sine_table):
    half = values.shape[-1] // 2
    lo, hi = values[..., :half], values[..., half:]
    return jnp.concatenate([lo * cosine - hi * sine_table, hi * cosine + lo * sine_table], -1)


CHUNKS = (
    (("mine", "own"), ("peer", "own")),
    (("mine", "up"), ("mine", "down"), ("peer", "up"), ("peer", "down")),
    (("mine", "far"), ("peer", "far")),
)
SPANS_PER_PIECE = 16
PIECE_ROWS = SPANS_PER_PIECE * SPAN
VMEM_LIMIT = 20 << 20
LIST_PAD = 16
BLOCK = 1024
SHARD = 32
PACK = SHARD * 576 // 128


def list_len(chunk):
    return len(chunk) * SPANS_PER_PIECE + LIST_PAD


def plan_kernel(order_ref, here_ref, *lists):
    x, y, core, seq = here_ref[0], here_ref[1], here_ref[2], here_ref[3]
    mine = [order_ref[2 * seq + q] for q in range(2)]
    floors = [jnp.bitwise_and(g, -64) for g in mine]
    for chunk, out in zip(CHUNKS, lists):
        length = list_len(chunk)
        counts = [jnp.int32(0), jnp.int32(0)]
        diags = [jnp.int32(0), jnp.int32(0)]
        for n, (side, name) in enumerate(chunk):
            on = core if side == "mine" else 1 - core
            fixed_x = jnp.bitwise_and(x + (SHIFTS[name] + NX), NX - 1)
            fixed_y = jnp.bitwise_and(y + (SHIFTS[name] + NY), NY - 1)
            base = jnp.where(on == 0, fixed_y * 4, fixed_x * 32 + 2)
            stride = jnp.where(on == 0, 32, 4)
            for a in range(4):
                start = base + stride * a
                for zp in range(4):
                    g = order_ref[start + (zp // 2) * 16 + zp % 2]
                    row = n * SPANS_PER_PIECE + a * 4 + zp
                    for q in range(2):
                        out[q * length + counts[q]] = row
                        full = jnp.logical_and(g >= floors[q], g < mine[q])
                        counts[q] = counts[q] + full.astype(jnp.int32)
                        diags[q] = jnp.where(g == mine[q], row, diags[q])
        for q in range(2):
            for k in range(LIST_PAD):
                out[q * length + counts[q] + k] = diags[q] if k == 0 else 0
            out[2 * length + q] = counts[q]


def plan(order, here):
    smem = pl.BlockSpec(memory_space=pltpu.SMEM)
    return pl.pallas_call(
        plan_kernel,
        out_shape=[jax.ShapeDtypeStruct((2 * list_len(ch) + 2,), jnp.int32) for ch in CHUNKS],
        in_specs=[smem, smem],
        out_specs=[smem] * len(CHUNKS),
        name="plan",
    )(order, here)


def turn(pair, cosine, sine_table):
    lane = lax.broadcasted_iota(jnp.int32, pair.shape, pair.ndim - 1)
    swapped = jnp.where(
        jnp.bitwise_and(lane, 32) == 0,
        pltpu.roll(pair, 96, pair.ndim - 1),
        pltpu.roll(pair, 32, pair.ndim - 1),
    )
    return pair * cosine + swapped * sine_table


def prepare_kernel(queries_ref, cos_ref, sin_ref, out_ref):
    rows = queries_ref.shape[0]
    span_rows = rows // 2
    width = out_ref.shape[2]
    rank = width - ROPE_DIM
    cosine, sine_table = cos_ref[...], sin_ref[...]
    lane = lax.broadcasted_iota(jnp.int32, (rows, 128), 1)
    low = lane < 64
    for pair in range(queries_ref.shape[1] // (2 * width)):
        at = 2 * width * pair

        def block(k, at=at):
            return queries_ref[:, at + 128 * k : at + 128 * (k + 1)]

        blocks = [block(k) for k in range(2 * width // 128)]
        mid = rank // 128
        shifted = [pltpu.roll(b.astype(jnp.float32), 64, 1) for b in blocks[mid:]]
        ropes = jnp.where(low, blocks[mid].astype(jnp.float32), blocks[-1].astype(jnp.float32))
        ropes = turn(ropes, cosine, sine_table)
        tails = [ropes.astype(jnp.bfloat16), pltpu.roll(ropes, 64, 1).astype(jnp.bfloat16)]
        bodies = [
            blocks[:mid],
            [jnp.where(low, shifted[k], shifted[k + 1]).astype(jnp.bfloat16) for k in range(mid)],
        ]
        for odd in range(2):
            head = 2 * pair + odd
            for q in range(2):
                part = slice(q * span_rows, (q + 1) * span_rows)
                dst = slice(head * span_rows, (head + 1) * span_rows)
                for k in range(mid):
                    out_ref[q, dst, 128 * k : 128 * (k + 1)] = bodies[odd][k][part]
                out_ref[q, dst, rank:width] = tails[odd][part, :ROPE_DIM]


def prepare(queries, cosine, sine_table, heads):
    vmem = pl.BlockSpec(memory_space=pltpu.VMEM)
    rows, lanes = queries.shape
    width = lanes // heads
    return pl.pallas_call(
        prepare_kernel,
        out_shape=jax.ShapeDtypeStruct((2, heads * rows // 2, width), jnp.bfloat16),
        in_specs=[vmem] * 3,
        out_specs=vmem,
        cost_estimate=pl.CostEstimate(flops=4 << 30, bytes_accessed=6 << 20, transcendentals=0),
        compiler_params=pltpu.CompilerParams(vmem_limit_bytes=16 << 20),
        name="prepare",
    )(queries, cosine, sine_table)


def attend_kernel(n_pieces, first, last, scale, *refs):
    refs = list(refs)
    lists, q_ref = refs.pop(0), refs.pop(0)
    pieces = [refs.pop(0) for _ in range(n_pieces)]
    if not first:
        acc_in, top_in, tot_in = refs.pop(0), refs.pop(0), refs.pop(0)
    if last:
        w_ref, out_ref = refs.pop(0), refs.pop(0)
        acc_ref, top_ref, tot_ref = acc_in, top_in, tot_in
    else:
        acc_ref, top_ref, tot_ref = refs.pop(0), refs.pop(0), refs.pop(0)
    kbuf, rope_buf, s_buf, sems = refs
    shards = PIECE_ROWS // SHARD
    rank = kbuf.shape[2] - ROPE_DIM
    rows = q_ref.shape[1]
    copies = []
    for i, piece in enumerate(pieces):
        own = []
        dst = pl.ds(i * shards, shards)
        for b in range(rank // 128):
            own.append(
                pltpu.make_async_copy(
                    piece.at[:, pl.ds(b * SHARD, SHARD), :], kbuf.at[dst, :, pl.ds(b * 128, 128)], sems.at[i, b]
                )
            )
        own.append(
            pltpu.make_async_copy(
                piece.at[:, pl.ds(rank // 128 * SHARD, SHARD // 2), :], rope_buf.at[dst], sems.at[i, rank // 128]
            )
        )
        copies.append(own)
    for own in copies:
        for cp in own:
            cp.start()
    if first:
        acc_ref[...] = jnp.zeros_like(acc_ref)
        top_ref[...] = jnp.full_like(top_ref, -jnp.inf)
        tot_ref[...] = jnp.zeros_like(tot_ref)
    for i, own in enumerate(copies):
        for cp in own:
            cp.wait()
        dst = pl.ds(i * shards, shards)
        packed = rope_buf[dst]
        kbuf[dst, pl.ds(0, SHARD // 2), pl.ds(rank, ROPE_DIM)] = packed[:, :, :ROPE_DIM]
        kbuf[dst, pl.ds(SHARD // 2, SHARD // 2), pl.ds(rank, ROPE_DIM)] = packed[:, :, ROPE_DIM:]

    length = n_pieces * SPANS_PER_PIECE + LIST_PAD
    counts = [lists[2 * length + q] for q in range(2)]
    extra = 1 if first else 0
    items = [lax.shift_right_logical(n + (extra + SLOTS - 1), SLOTS.bit_length() - 1) for n in counts]

    def locate(i):
        q = (i >= items[0]).astype(jnp.int32)
        return q, i - q * items[0]

    def keys(q, i):
        tiles = [kbuf[pl.ds(lists[q * length + i * SLOTS + k] * 2, 2)] for k in range(SLOTS)]
        return jnp.concatenate(tiles, 0).reshape(TILE, kbuf.shape[2])

    def score(q, tile, block):
        part = pl.ds(block * BLOCK, BLOCK)
        s_buf[part, :] = lax.dot_general(
            q_ref[q, part, :], tile, (((1,), (1,)), ((), ())), preferred_element_type=jnp.float32
        )

    cols = lax.broadcasted_iota(jnp.int32, (SPAN, TILE), 1)
    toks = lax.broadcasted_iota(jnp.int32, (SPAN, TILE), 0)
    ahead = cols - toks if first else cols + 1
    total_items = items[0] + items[1]

    @pl.when(total_items > 0)
    def _():
        q, at = locate(0)
        tile = keys(q, at)
        for block in range(rows // BLOCK):
            score(q, tile, block)

    def step(i, carry):
        q, at = locate(i)
        q_next, at_next = locate(i + 1)
        tile_next = keys(q_next, at_next)
        count = jnp.where(q == 0, counts[0], counts[1])
        visible = ahead <= SPAN * (count - SLOTS * at)
        values = keys(q, at)[:, :rank]
        for block in range(rows // BLOCK):
            probs, alphas = [], []
            for h in range(block * BLOCK // SPAN, (block + 1) * BLOCK // SPAN):
                part = pl.ds(h * SPAN, SPAN)
                s = jnp.where(visible, s_buf[part, :] * scale, -jnp.inf)
                old = top_ref[q, part, :]
                new = jnp.maximum(old, jnp.max(s, 1, keepdims=True))
                top_ref[q, part, :] = new
                alpha = jnp.exp2(old - new)
                p = jnp.exp2(s - jnp.concatenate([new] * (TILE // 128), 1))
                sums = p[:, :128]
                for b in range(1, TILE // 128):
                    sums = sums + p[:, b * 128 : (b + 1) * 128]
                tot_ref[q, part, :] = tot_ref[q, part, :] * alpha + sums
                probs.append(p.astype(jnp.bfloat16))
                alphas.append(alpha)
            score(q_next, tile_next, block)
            contrib = jnp.dot(jnp.concatenate(probs, 0), values, preferred_element_type=jnp.float32)
            alpha = jnp.concatenate(alphas, 0)
            part = pl.ds(block * BLOCK, BLOCK)
            for b in range(rank // 128):
                lanes = pl.ds(b * 128, 128)
                acc_ref[q, part, lanes] = acc_ref[q, part, lanes] * alpha + contrib[:, b * 128 : (b + 1) * 128]
        return carry

    lax.fori_loop(0, total_items, step, 0)
    if last:
        for q in range(2):
            for h in range(rows // SPAN):
                part = pl.ds(h * SPAN, SPAN)
                total = jnp.sum(tot_ref[q, part, :], 1, keepdims=True)
                latent = (acc_ref[q, part, :] / total).astype(jnp.bfloat16)
                out = jnp.dot(latent, w_ref[h], preferred_element_type=jnp.float32)
                out_ref[pl.ds(q * SPAN, SPAN), pl.ds(h * 128, 128)] = out.astype(jnp.bfloat16)


def attend(lists, q, pieces, state, w_uv, scale):
    first, last = state is None, w_uv is not None
    vmem = pl.BlockSpec(memory_space=pltpu.VMEM)
    smem = pl.BlockSpec(memory_space=pltpu.SMEM)
    hbm = pl.BlockSpec(memory_space=pl.ANY)
    spans, rows, width = q.shape
    rank = width - ROPE_DIM
    args = [lists, q, *pieces]
    in_specs = [smem, vmem] + [hbm] * len(pieces)
    aliases = {}
    if not first:
        if not last:
            aliases = {len(args) + k: k for k in range(3)}
        args += list(state)
        in_specs += [vmem] * 3
    if last:
        args.append(w_uv)
        in_specs.append(vmem)
        out_shape = jax.ShapeDtypeStruct((spans * SPAN, w_uv.shape[0] * w_uv.shape[2]), jnp.bfloat16)
        out_specs = vmem
    else:
        out_shape = [
            jax.ShapeDtypeStruct((spans, rows, rank), jnp.float32),
            jax.ShapeDtypeStruct((spans, rows, 128), jnp.float32),
            jax.ShapeDtypeStruct((spans, rows, 128), jnp.float32),
        ]
        out_specs = [vmem] * 3
    n = len(pieces)
    flops = n * rows * PIECE_ROWS * (width + rank) * 2
    return pl.pallas_call(
        functools.partial(attend_kernel, n, first, last, scale),
        out_shape=out_shape,
        in_specs=in_specs,
        out_specs=out_specs,
        scratch_shapes=[
            pltpu.VMEM((n * PIECE_ROWS // SHARD, SHARD, width), jnp.bfloat16),
            pltpu.VMEM((n * PIECE_ROWS // SHARD, SHARD // 2, 128), jnp.bfloat16),
            pltpu.VMEM((rows, TILE), jnp.float32),
            pltpu.SemaphoreType.DMA((n, rank // 128 + 1)),
        ],
        input_output_aliases=aliases,
        cost_estimate=pl.CostEstimate(flops=flops, bytes_accessed=8 << 20, transcendentals=n * rows * PIECE_ROWS),
        compiler_params=pltpu.CompilerParams(vmem_limit_bytes=VMEM_LIMIT),
        name="attend_" + ("first" if first else "last" if last else "middle"),
    )(*args)


def per_device(span_order, queries, latent_kv, w_uv):
    tok_dev = queries.shape[0]
    head_count, latent_rank, _ = w_uv.shape
    row_width = queries.shape[1] // head_count
    rope_width = row_width - latent_rank
    seq, head = lax.axis_index("seq"), lax.axis_index("head")
    core, y, x = seq % NC, (seq // NC) % NY, seq // (NC * NY * (NZ // ZL))
    seq_len = tok_dev * lax.axis_size("seq") // SEQS

    kv_count = latent_kv.shape[0]
    mine = lax.dynamic_slice_in_dim(span_order, 2 * seq, 2)
    positions = (mine[:, None] * SPAN + jnp.arange(SPAN, dtype=jnp.int32)[None, :]).reshape(-1) % seq_len
    cos_q, sin_q = angle_tables(positions, rope_width // 2)
    cos_k = lax.dynamic_slice_in_dim(cos_q, head * kv_count, kv_count)
    sin_k = lax.dynamic_slice_in_dim(sin_q, head * kv_count, kv_count)
    rope = rotate(latent_kv[:, latent_rank:].astype(jnp.float32), cos_k, sin_k).astype(jnp.bfloat16)
    packed = jnp.concatenate(
        [latent_kv[:, 128 * b : 128 * (b + 1)] for b in range(latent_rank // 128)]
        + [jnp.concatenate([rope[: kv_count // 2], rope[kv_count // 2 :]], 1)],
        0,
    )[None]
    got = {("mine", "own"): collect(collect(packed, GROUP_Z), GROUP_A)}
    own = got["mine", "own"]
    for name in ("up", "down", "far"):
        got["mine", name] = permute(own, second_axis(-SHIFTS[name]))
    got["peer", "own"] = permute(own, other_core)

    here = jnp.stack([x, y, core, seq]).astype(jnp.int32)
    lists = plan(span_order, here)
    q = prepare(
        queries,
        jnp.concatenate([cos_q] * 4, 1),
        jnp.concatenate([-sin_q, sin_q] * 2, 1),
        head_count,
    )

    scale = (NOPE_DIM + ROPE_DIM) ** -0.5 * math.log2(math.e)
    state = attend(lists[0], q, [got[key] for key in CHUNKS[0]], None, None, scale)
    for name in ("up", "down"):
        got["mine", name], state = lax.optimization_barrier((got["mine", name], state))
        got["peer", name] = permute(got["mine", name], other_core)
    state = attend(lists[1], q, [got[key] for key in CHUNKS[1]], state, None, scale)
    got["peer", "far"] = permute(got["mine", "far"], other_core)
    state = attend(lists[2], q, [got[key] for key in CHUNKS[2]], state, w_uv, scale)
    return state


def solution(mesh):
    in_specs = (P(), P("seq", "head"), P(("seq", "head"), None), P("head", None, None))
    return jax.shard_map(
        per_device, mesh=mesh, in_specs=in_specs, out_specs=P("seq", "head"), check_vma=False
    )
```

```python
import functools
import math

import jax
import jax.numpy as jnp
from jax import lax
from jax.experimental import pallas as pl
from jax.experimental.pallas import tpu as pltpu
from jax.sharding import PartitionSpec as P

ROPE_DIM = 64
NOPE_DIM = 128
SEQS = 2
AXES = ("seq", "head")
NX, NY, NZ, NC = 4, 4, 8, 2
ZL = 4
SPAN = 64
SLOTS = 4
TILE = SLOTS * SPAN
THETA = 10000.0

SHIFTS = {"own": 0, "up": -1, "down": 1, "far": 2}


def place(x, y, z, c):
    return (((x * (NZ // ZL) + z // ZL) * NY + y) * NC + c) * ZL + z % ZL


def chips():
    return [(x, y, z, c) for x in range(NX) for y in range(NY) for z in range(NZ) for c in range(NC)]


def permute(value, target):
    pairs = [(place(*d), place(*target(*d))) for d in chips()]
    return lax.ppermute(value, AXES, pairs)


def first_axis(step):
    return lambda x, y, z, c: ((x + step) % NX, y, z, c) if c == 0 else (x, (y + step) % NY, z, c)


def second_axis(step):
    return lambda x, y, z, c: ((x + step) % NX, y, z, c) if c == 1 else (x, (y + step) % NY, z, c)


def other_core(x, y, z, c):
    return (x, y, z, 1 - c)


GROUP_Z = [[place(x, y, z, c) for z in range(NZ)] for x in range(NX) for y in range(NY) for c in range(NC)]

STEPS = (0, -1, 1, 2)


def turn_tables(positions):
    half = ROPE_DIM // 2
    lane = lax.broadcasted_iota(jnp.int32, positions.shape, positions.ndim - 1)
    order = jnp.bitwise_and(lane, half - 1).astype(jnp.float32)
    phases = positions.astype(jnp.float32) * jnp.exp(-math.log(THETA) * order / half)
    sine_table = jnp.sin(phases)
    return jnp.cos(phases), jnp.where(jnp.bitwise_and(lane, half) == 0, -sine_table, sine_table)


CHUNKS = (
    (("mine", "own"), ("peer", "own")),
    (("mine", "up"), ("mine", "down")),
    (("peer", "up"), ("peer", "down")),
    (("mine", "far"), ("peer", "far")),
)
SPANS_PER_PIECE = 16
PIECE_ROWS = SPANS_PER_PIECE * SPAN
VMEM_LIMIT = 20 << 20
LIST_PAD = 16
BLOCK = 1024
SHARD = 32
PACK = SHARD * 576 // 128


def list_len(chunk):
    return len(chunk) * SPANS_PER_PIECE + LIST_PAD


def plan(order_ref, lists):
    seq = lax.axis_index("seq")
    core = jnp.bitwise_and(seq, NC - 1)
    y = jnp.bitwise_and(lax.shift_right_logical(seq, 1), NY - 1)
    x = lax.shift_right_logical(seq, 4)
    mine = [order_ref[2 * seq + q] for q in range(2)]
    floors = [jnp.bitwise_and(g, -64) for g in mine]
    for chunk, out in zip(CHUNKS, lists):
        length = list_len(chunk)
        counts = [jnp.int32(0), jnp.int32(0)]
        diags = [jnp.int32(0), jnp.int32(0)]
        for n, (side, name) in enumerate(chunk):
            on = core if side == "mine" else 1 - core
            fixed_x = jnp.bitwise_and(x + (SHIFTS[name] + NX), NX - 1)
            fixed_y = jnp.bitwise_and(y + (SHIFTS[name] + NY), NY - 1)
            base = jnp.where(on == 0, fixed_y * 4, fixed_x * 32 + 2)
            stride = jnp.where(on == 0, 32, 4)
            along = jnp.where(on == 0, x, y)
            for j, step in enumerate(STEPS):
                start = base + stride * jnp.bitwise_and(along + (step + 4), 3)
                for zp in range(4):
                    g = order_ref[start + (zp // 2) * 16 + zp % 2]
                    row = n * SPANS_PER_PIECE + j * 4 + zp
                    for q in range(2):
                        out[q * length + counts[q]] = row
                        full = jnp.logical_and(g >= floors[q], g < mine[q])
                        counts[q] = counts[q] + full.astype(jnp.int32)
                        diags[q] = jnp.where(g == mine[q], row, diags[q])
        for q in range(2):
            for k in range(LIST_PAD):
                out[q * length + counts[q] + k] = diags[q] if k == 0 else 0
            out[2 * length + q] = counts[q]


def turn(pair, cosine, sine_table):
    lane = lax.broadcasted_iota(jnp.int32, pair.shape, pair.ndim - 1)
    swapped = jnp.where(
        jnp.bitwise_and(lane, 32) == 0,
        pltpu.roll(pair, 96, pair.ndim - 1),
        pltpu.roll(pair, 32, pair.ndim - 1),
    )
    return pair * cosine + swapped * sine_table


def prepare_kernel(seq_spans, order_ref, queries_ref, out_ref, *lists):
    plan(order_ref, lists)
    rows = queries_ref.shape[0]
    span_rows = rows // 2
    width = out_ref.shape[2]
    rank = width - ROPE_DIM
    seq = lax.axis_index("seq")
    row = lax.broadcasted_iota(jnp.int32, (rows, 128), 0)
    starts = [jnp.bitwise_and(order_ref[2 * seq + q], seq_spans - 1) * SPAN for q in range(2)]
    cosine, sine_table = turn_tables(jnp.where(row < span_rows, row + starts[0], row + (starts[1] - span_rows)))
    low = lax.broadcasted_iota(jnp.int32, (rows, 128), 1) < 64
    for pair in range(queries_ref.shape[1] // (2 * width)):
        at = 2 * width * pair

        def block(k, at=at):
            return queries_ref[:, at + 128 * k : at + 128 * (k + 1)]

        blocks = [block(k) for k in range(2 * width // 128)]
        mid = rank // 128
        shifted = [pltpu.roll(b.astype(jnp.float32), 64, 1) for b in blocks[mid:]]
        ropes = jnp.where(low, blocks[mid].astype(jnp.float32), blocks[-1].astype(jnp.float32))
        ropes = turn(ropes, cosine, sine_table)
        tails = [ropes.astype(jnp.bfloat16), pltpu.roll(ropes, 64, 1).astype(jnp.bfloat16)]
        bodies = [
            blocks[:mid],
            [jnp.where(low, shifted[k], shifted[k + 1]).astype(jnp.bfloat16) for k in range(mid)],
        ]
        for odd in range(2):
            head = 2 * pair + odd
            for q in range(2):
                part = slice(q * span_rows, (q + 1) * span_rows)
                dst = slice(head * span_rows, (head + 1) * span_rows)
                for k in range(mid):
                    out_ref[q, dst, 128 * k : 128 * (k + 1)] = bodies[odd][k][part]
                out_ref[q, dst, rank:width] = tails[odd][part, :ROPE_DIM]


def prepare(order, queries, heads, seq_spans):
    vmem = pl.BlockSpec(memory_space=pltpu.VMEM)
    smem = pl.BlockSpec(memory_space=pltpu.SMEM)
    rows, lanes = queries.shape
    width = lanes // heads
    return pl.pallas_call(
        functools.partial(prepare_kernel, seq_spans),
        out_shape=[jax.ShapeDtypeStruct((2, heads * rows // 2, width), jnp.bfloat16)]
        + [jax.ShapeDtypeStruct((2 * list_len(ch) + 2,), jnp.int32) for ch in CHUNKS],
        in_specs=[smem, vmem],
        out_specs=[vmem] + [smem] * len(CHUNKS),
        cost_estimate=pl.CostEstimate(flops=4 << 30, bytes_accessed=6 << 20, transcendentals=0),
        compiler_params=pltpu.CompilerParams(vmem_limit_bytes=16 << 20),
        name="prepare",
    )(order, queries)


def pack_kernel(seq_spans, order_ref, latent_hbm, out_ref, latent_ref, sem):
    load = pltpu.make_async_copy(latent_hbm, latent_ref, sem)
    load.start()
    rows, width = latent_ref.shape
    rank = width - ROPE_DIM
    seq, head = lax.axis_index("seq"), lax.axis_index("head")
    home = order_ref[2 * seq + lax.shift_right_logical(head, 1)]
    start = jnp.bitwise_and(home, seq_spans - 1) * SPAN + jnp.bitwise_and(head, 1) * rows
    row = lax.broadcasted_iota(jnp.int32, (rows // 2, 128), 0)
    lane = lax.broadcasted_iota(jnp.int32, (rows // 2, 128), 1)
    cosine, sine_table = turn_tables(start + row + jnp.where(lane < ROPE_DIM, 0, rows // 2))
    load.wait()
    rope = latent_ref[:, rank:].astype(jnp.float32)
    pair = jnp.concatenate([rope[: rows // 2], rope[rows // 2 :]], 1)
    pair = turn(pair, cosine, sine_table).astype(jnp.bfloat16)
    for k in range(out_ref.shape[0]):
        for b in range(rank // 128):
            out_ref[k, b * rows : (b + 1) * rows, :] = latent_ref[:, b * 128 : (b + 1) * 128]
        out_ref[k, rank // 128 * rows :, :] = pair


def pack(order, latent, copies, seq_spans):
    rows, width = latent.shape
    return pl.pallas_call(
        functools.partial(pack_kernel, seq_spans),
        out_shape=jax.ShapeDtypeStruct((copies, rows * width // 128, 128), jnp.bfloat16),
        in_specs=[pl.BlockSpec(memory_space=pltpu.SMEM), pl.BlockSpec(memory_space=pl.ANY)],
        out_specs=pl.BlockSpec(memory_space=pltpu.VMEM),
        scratch_shapes=[pltpu.VMEM((rows, width), jnp.bfloat16), pltpu.SemaphoreType.DMA],
        compiler_params=pltpu.CompilerParams(vmem_limit_bytes=4 << 20),
        name="pack",
    )(order, latent)


def attend_kernel(n_pieces, first, last, scale, *refs):
    refs = list(refs)
    lists, q_ref = refs.pop(0), refs.pop(0)
    pieces = [refs.pop(0) for _ in range(n_pieces)]
    if not first:
        acc_in, top_in, tot_in = refs.pop(0), refs.pop(0), refs.pop(0)
    if last:
        w_ref, out_ref = refs.pop(0), refs.pop(0)
        acc_ref, top_ref, tot_ref = acc_in, top_in, tot_in
    else:
        acc_ref, top_ref, tot_ref = refs.pop(0), refs.pop(0), refs.pop(0)
    kbuf, rope_buf, s_buf, sems = refs
    rank = kbuf.shape[2] - ROPE_DIM
    rows = q_ref.shape[1]
    copies, spots = [], []
    begin = 0
    for i, piece in enumerate(pieces):
        own = []
        dst = pl.ds(begin, piece.shape[0])
        begin += piece.shape[0]
        spots.append(dst)
        for b in range(rank // 128):
            own.append(
                pltpu.make_async_copy(
                    piece.at[:, pl.ds(b * SHARD, SHARD), :], kbuf.at[dst, :, pl.ds(b * 128, 128)], sems.at[i, b]
                )
            )
        own.append(
            pltpu.make_async_copy(
                piece.at[:, pl.ds(rank // 128 * SHARD, SHARD // 2), :], rope_buf.at[dst], sems.at[i, rank // 128]
            )
        )
        copies.append(own)
    for own in copies:
        for cp in own:
            cp.start()
    if first:
        acc_ref[...] = jnp.zeros_like(acc_ref)
        top_ref[...] = jnp.full_like(top_ref, -jnp.inf)
        tot_ref[...] = jnp.zeros_like(tot_ref)
    for i, own in enumerate(copies):
        for cp in own:
            cp.wait()
        dst = spots[i]
        packed = rope_buf[dst]
        kbuf[dst, pl.ds(0, SHARD // 2), pl.ds(rank, ROPE_DIM)] = packed[:, :, :ROPE_DIM]
        kbuf[dst, pl.ds(SHARD // 2, SHARD // 2), pl.ds(rank, ROPE_DIM)] = packed[:, :, ROPE_DIM:]

    length = kbuf.shape[0] * SHARD // SPAN + LIST_PAD
    counts = [lists[2 * length + q] for q in range(2)]
    extra = 1 if first else 0
    items = [lax.shift_right_logical(n + (extra + SLOTS - 1), SLOTS.bit_length() - 1) for n in counts]

    def locate(i):
        q = (i >= items[0]).astype(jnp.int32)
        return q, i - q * items[0]

    def keys(q, i):
        tiles = [kbuf[pl.ds(lists[q * length + i * SLOTS + k] * 2, 2)] for k in range(SLOTS)]
        return jnp.concatenate(tiles, 0).reshape(TILE, kbuf.shape[2])

    def score(q, tile, block):
        part = pl.ds(block * BLOCK, BLOCK)
        s_buf[part, :] = lax.dot_general(
            q_ref[q, part, :], tile, (((1,), (1,)), ((), ())), preferred_element_type=jnp.float32
        )

    cols = lax.broadcasted_iota(jnp.int32, (SPAN, TILE), 1)
    toks = lax.broadcasted_iota(jnp.int32, (SPAN, TILE), 0)
    ahead = cols - toks if first else cols + 1
    total_items = items[0] + items[1]

    @pl.when(total_items > 0)
    def _():
        q, at = locate(0)
        tile = keys(q, at)
        for block in range(rows // BLOCK):
            score(q, tile, block)

    def step(i, carry):
        q, at = locate(i)
        q_next, at_next = locate(i + 1)
        tile_next = keys(q_next, at_next)
        count = jnp.where(q == 0, counts[0], counts[1])
        visible = ahead <= SPAN * (count - SLOTS * at)
        values = keys(q, at)[:, :rank]
        for block in range(rows // BLOCK):
            probs, alphas = [], []
            for h in range(block * BLOCK // SPAN, (block + 1) * BLOCK // SPAN):
                part = pl.ds(h * SPAN, SPAN)
                s = jnp.where(visible, s_buf[part, :] * scale, -jnp.inf)
                old = top_ref[q, part, :]
                new = jnp.maximum(old, jnp.max(s, 1, keepdims=True))
                top_ref[q, part, :] = new
                alpha = jnp.exp2(old - new)
                p = jnp.exp2(s - jnp.concatenate([new] * (TILE // 128), 1))
                sums = p[:, :128]
                for b in range(1, TILE // 128):
                    sums = sums + p[:, b * 128 : (b + 1) * 128]
                tot_ref[q, part, :] = tot_ref[q, part, :] * alpha + sums
                probs.append(p.astype(jnp.bfloat16))
                alphas.append(alpha)
            score(q_next, tile_next, block)
            contrib = jnp.dot(jnp.concatenate(probs, 0), values, preferred_element_type=jnp.float32)
            alpha = jnp.concatenate(alphas, 0)
            part = pl.ds(block * BLOCK, BLOCK)
            for b in range(rank // 128):
                lanes = pl.ds(b * 128, 128)
                acc_ref[q, part, lanes] = acc_ref[q, part, lanes] * alpha + contrib[:, b * 128 : (b + 1) * 128]
        return carry

    lax.fori_loop(0, total_items, step, 0)
    if last:
        for q in range(2):
            for h in range(rows // SPAN):
                part = pl.ds(h * SPAN, SPAN)
                total = jnp.sum(tot_ref[q, part, :], 1, keepdims=True)
                latent = (acc_ref[q, part, :] / total).astype(jnp.bfloat16)
                out = jnp.dot(latent, w_ref[h], preferred_element_type=jnp.float32)
                out_ref[pl.ds(q * SPAN, SPAN), pl.ds(h * 128, 128)] = out.astype(jnp.bfloat16)


def attend(lists, q, pieces, state, w_uv, scale):
    first, last = state is None, w_uv is not None
    vmem = pl.BlockSpec(memory_space=pltpu.VMEM)
    smem = pl.BlockSpec(memory_space=pltpu.SMEM)
    hbm = pl.BlockSpec(memory_space=pl.ANY)
    spans, rows, width = q.shape
    rank = width - ROPE_DIM
    args = [lists, q, *pieces]
    in_specs = [smem, vmem] + [hbm] * len(pieces)
    aliases = {}
    if not first:
        if not last:
            aliases = {len(args) + k: k for k in range(3)}
        args += list(state)
        in_specs += [vmem] * 3
    if last:
        args.append(w_uv)
        in_specs.append(vmem)
        out_shape = jax.ShapeDtypeStruct((spans * SPAN, w_uv.shape[0] * w_uv.shape[2]), jnp.bfloat16)
        out_specs = vmem
    else:
        out_shape = [
            jax.ShapeDtypeStruct((spans, rows, rank), jnp.float32),
            jax.ShapeDtypeStruct((spans, rows, 128), jnp.float32),
            jax.ShapeDtypeStruct((spans, rows, 128), jnp.float32),
        ]
        out_specs = [vmem] * 3
    n = sum(p.shape[0] for p in pieces) * SHARD // PIECE_ROWS
    flops = n * rows * PIECE_ROWS * (width + rank) * 2
    return pl.pallas_call(
        functools.partial(attend_kernel, len(pieces), first, last, scale),
        out_shape=out_shape,
        in_specs=in_specs,
        out_specs=out_specs,
        scratch_shapes=[
            pltpu.VMEM((n * PIECE_ROWS // SHARD, SHARD, width), jnp.bfloat16),
            pltpu.VMEM((n * PIECE_ROWS // SHARD, SHARD // 2, 128), jnp.bfloat16),
            pltpu.VMEM((rows, TILE), jnp.float32),
            pltpu.SemaphoreType.DMA((len(pieces), rank // 128 + 1)),
        ],
        input_output_aliases=aliases,
        cost_estimate=pl.CostEstimate(flops=flops, bytes_accessed=8 << 20, transcendentals=n * rows * PIECE_ROWS),
        compiler_params=pltpu.CompilerParams(vmem_limit_bytes=VMEM_LIMIT),
        name="attend_" + ("first" if first else "last" if last else "middle"),
    )(*args)


def per_device(span_order, queries, latent_kv, w_uv):
    tok_dev = queries.shape[0]
    head_count, latent_rank, _ = w_uv.shape
    seq_spans = tok_dev * lax.axis_size("seq") // SEQS // SPAN

    copies = pack(span_order, latent_kv, NZ, seq_spans)
    column = lax.all_to_all(copies, AXES, split_axis=0, concat_axis=0, tiled=True, axis_index_groups=GROUP_Z)
    parts = [column] + [permute(column, first_axis(-step)) for step in STEPS[1:]]
    q, *lists = prepare(span_order, queries, head_count, seq_spans)
    *parts, q = lax.optimization_barrier((*parts, q))
    own = jnp.concatenate(parts, 0)
    got = {("mine", "own"): own}
    for name in ("up", "down"):
        got["mine", name] = permute(own, second_axis(-SHIFTS[name]))
    got["peer", "own"] = permute(own, other_core)

    scale = (NOPE_DIM + ROPE_DIM) ** -0.5 * math.log2(math.e)
    state = attend(lists[0], q, [got[key] for key in CHUNKS[0]], None, None, scale)
    up, down, state = lax.optimization_barrier((got["mine", "up"], got["mine", "down"], state))
    half = up.shape[0] // 2
    far = [permute(up[:half], second_axis(1)), permute(down[half:], second_axis(-1))]
    peers = [permute(piece, other_core) for piece in (up, down)]
    state = attend(lists[1], q, [up, down], state, None, scale)
    *far, state = lax.optimization_barrier((*far, state))
    far = far + [permute(piece, other_core) for piece in far]
    state = attend(lists[2], q, peers, state, None, scale)
    return attend(lists[3], q, far, state, w_uv, scale)


def solution(mesh):
    in_specs = (P(), P("seq", "head"), P(("seq", "head"), None), P("head", None, None))
    return jax.shard_map(
        per_device, mesh=mesh, in_specs=in_specs, out_specs=P("seq", "head"), check_vma=False
    )
```
